32 devices in a mesh: row: 4 (over y, x), col: 8 (over z, core).
Axes of the slice: x: 2, y: 2, z: 4, core: 2. Of those that a mesh axis runs over, the one named last changes fastest.
Arguments:
- fire_state: float32 [64, 192, 1024], P(None, 'row', 'col'), may hold values from -6 to 6
- fuel_class: int32 [192, 1024], P('row', 'col'), may hold values from 0 to 12
- firebreak: int32 [192, 1024], P('row', 'col'), may hold values 0 or 1
- ignition: int32 [192, 1024], P('row', 'col'), may hold values 0 or 1
- spread_rate: float32 [13, 64], replicated, may hold values from 0.03 to 0.12
- spread_rows: float32 [64, 64], replicated, may hold values from -0.375 to 0.375
- spread_cols: float32 [64, 64], replicated, may hold values from -0.375 to 0.375
- reaction: float32 [64, 64], replicated, may hold values from -0.75 to 0.75
- ignition_heat: float32 [64], replicated, may hold values from -4 to 4
Outputs:
- final_state: float32 [64, 192, 1024], P(None, 'row', 'col')
The draws below stay inside these ranges and needn't reach their ends.
All inputs are finite; a program needn't handle non-finite values. No bound on the sum of `firebreak` or of `ignition` on one device may be relied on, other than what follows from the above.
Results may differ from the reference program's by a relative error of at most 0.0003.
Values sent between devices are 32-bit elements; how exact they have to be, the bound alone decides.
A program may use at most 64 MiB of HBM per device.

```python
import math
import jax
import jax.numpy as jnp
from jax import lax

C = 64
K = 13
W_DEV = 128
ITERS = 4
NX = 192
NY = 1024


def touch_ends(drawn, stream_key, low, largest):
    index_at = [jax.random.randint(jax.random.fold_in(stream_key, axis), (), 0, length) for axis, length in enumerate(drawn.shape)]
    main_axis = drawn.shape.index(max(drawn.shape))
    beside = index_at[:main_axis] + [(index_at[main_axis] + 1) % drawn.shape[main_axis]] + index_at[main_axis + 1:]
    return drawn.at[tuple(index_at)].set(low).at[tuple(beside)].set(largest)


def shard_levels(stream_key, dims, shards, smallest, high):
    gain = 1.0
    for axis_at, blocks in shards:
        heights = jax.random.uniform(jax.random.fold_in(jax.random.fold_in(stream_key, 6), axis_at), (blocks,), jnp.float32, smallest / len(shards), high / len(shards))
        gain = gain * jnp.repeat(jnp.exp(heights), dims[axis_at] // blocks).reshape((-1,) + (1,) * (len(dims) - 1 - axis_at))
    return gain


def centred(rng, dims, scale, reach, cuts=(), kind=jnp.bfloat16):
    array = jax.random.normal(rng, dims, jnp.float32) * scale
    if len(cuts) > 0:
        array = shard_levels(rng, dims, cuts, -0.22, 0.18) * array
    return jnp.clip(array, min=-reach, max=reach).astype(kind)


def setup_inputs(seed: int = 0) -> dict:
    key_list = jax.random.split(jax.random.key(seed), 10)
    fire_state = centred(key_list[0], (C, NX, NY), 1.0, 6.0, ((1, 4), (2, 8)), jnp.float32)
    fuel_class = touch_ends(jax.random.randint(key_list[1], (NX, NY), 0, K), jax.random.fold_in(key_list[1], 1), 0, K - 1).astype(jnp.int32)
    firebreak = touch_ends((jax.random.randint(key_list[2], (NX, NY), 0, 8) < 1).astype(jnp.int32), jax.random.fold_in(key_list[2], 1), 0, 1)
    ignition = touch_ends((jax.random.randint(key_list[3], (NX, NY), 0, 16) < 1).astype(jnp.int32), jax.random.fold_in(key_list[3], 1), 0, 1)
    spread_rate = jnp.clip(jnp.exp(jax.random.uniform(key_list[4], (K, C), jnp.float32, math.log(0.03), math.log(0.12))), 0.03, 0.12)
    spread_rows = centred(key_list[5], (C, C), (4 * C) ** -0.5, 0.375, (), jnp.float32)
    spread_cols = centred(key_list[6], (C, C), (4 * C) ** -0.5, 0.375, (), jnp.float32)
    reaction = centred(key_list[7], (C, C), C ** -0.5, 0.75, (), jnp.float32)
    ignition_heat = centred(key_list[8], (C,), 1.0, 4.0, (), jnp.float32)
    return dict(fire_state=fire_state, fuel_class=fuel_class, firebreak=firebreak, ignition=ignition, spread_rate=spread_rate, spread_rows=spread_rows, spread_cols=spread_cols, reaction=reaction, ignition_heat=ignition_heat)


def mixing(matrix, values):
    return jnp.einsum('dc,chw->dhw', matrix, values, precision=lax.Precision.HIGHEST)


def tendency(padded, burnable, spread, heating, spread_rows, spread_cols, reaction):
    center = padded[:, 1:-1, 1:-1]
    vertical = padded[:, :-2, 1:-1] + padded[:, 2:, 1:-1] - 2.0 * center
    horizontal = padded[:, 1:-1, :-2] + padded[:, 1:-1, 2:] - 2.0 * center
    mixed = vertical + mixing(spread_rows, vertical) + horizontal + mixing(spread_cols, horizontal)
    drive = spread * mixed + mixing(reaction, jnp.tanh(center)) + heating
    return burnable[None] * drive - 0.5 * center


def full_tendency(field, burnable_int, fuel_class, ignition, spread_rate, spread_rows, spread_cols, reaction, ignition_heat):
    padded = jnp.pad(field, ((0, 0), (1, 1), (1, 1)))
    blocks = NY // W_DEV

    def one_block(column_block):
        begin = column_block * W_DEV
        piece = lax.dynamic_slice_in_dim(padded, begin, W_DEV + 2, 2)
        burnable = lax.dynamic_slice_in_dim(burnable_int, begin, W_DEV, 1).astype(jnp.float32)
        fuel = lax.dynamic_slice_in_dim(fuel_class, begin, W_DEV, 1)
        lit = lax.dynamic_slice_in_dim(ignition, begin, W_DEV, 1).astype(jnp.float32)
        onehot = (fuel[None] == jnp.arange(K, dtype=jnp.int32)[:, None, None]).astype(jnp.float32)
        spread = jnp.einsum('kc,khw->chw', spread_rate, onehot, precision=lax.Precision.HIGHEST)
        heating = lit[None] * ignition_heat[:, None, None]
        return tendency(piece, burnable, spread, heating, spread_rows, spread_cols, reaction)

    result = lax.map(one_block, jnp.arange(blocks, dtype=jnp.int32))
    result = jnp.moveaxis(result, 0, 2)
    return result.reshape(C, NX, NY)


def reference(fire_state, fuel_class, firebreak, ignition, spread_rate, spread_rows, spread_cols, reaction, ignition_heat):
    burnable_int = 1 - firebreak
    field = fire_state
    for iteration in range(ITERS):
        first = full_tendency(field, burnable_int, fuel_class, ignition, spread_rate, spread_rows, spread_cols, reaction, ignition_heat)
        middle = field + first
        second = full_tendency(middle, burnable_int, fuel_class, ignition, spread_rate, spread_rows, spread_cols, reaction, ignition_heat)
        field = field + 0.5 * (first + second)
    return field
```

```python
import functools

import jax
import jax.numpy as jnp
from jax import lax
from jax.experimental import pallas as pl
from jax.experimental.pallas import tpu as pltpu
from jax.sharding import PartitionSpec as P

ITERS = 4
PAD = 8
BLOCK = 4
BF16, F32 = jnp.bfloat16, jnp.float32
MESH = pl.DeviceIdType.MESH


def split(x):
    high = x.astype(BF16)
    return high, (x - high.astype(F32)).astype(BF16)


def dot(a, b):
    return jnp.dot(a, b, preferred_element_type=F32)


def lanes(shape):
    return lax.broadcasted_iota(jnp.int32, shape, 1)


def rows_of(shape):
    return lax.broadcasted_iota(jnp.int32, shape, 0)


def on_diagonal(matrix):
    c = matrix.shape[0]
    turned = matrix.T
    wide = jnp.concatenate([turned, turned], axis=1)
    first = lanes(wide.shape) < c
    return jnp.concatenate([jnp.where(first, wide, 0.0), jnp.where(first, 0.0, wide)], axis=0)


def kernel(
    dims,
    x_ref, fuel_ref, break_ref, lit_ref, rate_ref, srow_ref, scol_ref, react_ref, heat_ref,
    out_ref,
    v, mid, local, coef, burn, heat, gr, gc, w1, w2, w3, wc, send_row, send_col, recv_row, recv_col, send_sem, recv_sem,
):
    n_row, n_col, c, h, w, k8 = dims
    p_all, half = h // 2, w // 2
    two = 2 * c
    r, q = lax.axis_index("row"), lax.axis_index("col")
    has_up, has_down = r > 0, r < n_row - 1
    has_left, has_right = q > 0, q < n_col - 1
    partner = ({"row": r - 1}, {"row": r + 1}, {"col": q - 1}, {"col": q + 1})
    sends = (has_up, has_down, has_left, has_right)
    takes = (has_down, has_up, has_right, has_left)

    recv_row[...] = jnp.zeros_like(recv_row)
    recv_col[...] = jnp.zeros_like(recv_col)
    barrier = pltpu.get_barrier_semaphore()
    for d in range(4):
        @pl.when(sends[d])
        def _(d=d):
            pl.semaphore_signal(barrier, inc=1, device_id=partner[d], device_id_type=MESH)

    def copy(slot, d):
        src, dst = (send_row, recv_row) if d < 2 else (send_col, recv_col)
        return pltpu.make_async_remote_copy(
            src_ref=src.at[slot, d % 2],
            dst_ref=dst.at[slot, d % 2],
            send_sem=send_sem.at[slot, d],
            recv_sem=recv_sem.at[slot, d],
            device_id=partner[d],
            device_id_type=MESH,
        )

    def start(slot, d):
        @pl.when(sends[d])
        def _():
            copy(slot, d).start()

    def finish(slot):
        for d in range(4):
            @pl.when(sends[d])
            def _(d=d):
                copy(slot, d).wait_send()
        for d in range(4):
            @pl.when(takes[d])
            def _(d=d):
                copy(slot, d).wait_recv()

    first_half = lanes((half, two)) < c

    def send_rows(slot, top, bottom):
        send_row[slot, 0] = jnp.where(first_half, top[:half], pltpu.roll(top[half:], c, axis=1))
        send_row[slot, 1] = jnp.where(first_half, pltpu.roll(bottom[:half], c, axis=1), bottom[half:])
        start(slot, 0)
        start(slot, 1)

    def turn_in(p):
        tall = jnp.concatenate([x_ref[pl.ds(p, c, stride=h), :], x_ref[pl.ds(p + p_all, c, stride=h), :]], axis=0)
        v[p] = tall.T

    def turn_in_loop(p, carry):
        turn_in(p)
        return carry

    lax.fori_loop(0, p_all, turn_in_loop, 0, unroll=4)

    def column(ref, at):
        size = ref.shape[1]
        flat = ref.reshape(ref.shape[0] * size, two)
        return lambda p: flat[pl.ds(p * size + at, p_all, stride=size), :]

    def send_cols(slot, left, right):
        send_col[slot, 0] = left
        send_col[slot, 1] = right
        start(slot, 2)
        start(slot, 3)

    n_near = sum(s.astype(jnp.int32) for s in sends)
    pl.semaphore_wait(barrier, n_near)
    send_rows(0, v[0], v[p_all - 1])
    send_cols(0, column(v, 0)(0), column(v, w - 1)(0))

    eye = (rows_of((two, two)) == lanes((two, two))).astype(F32)
    row_hi, row_lo = split(eye + on_diagonal(srow_ref[...]))
    col_hi, col_lo = split(eye + on_diagonal(scol_ref[...]))
    rea_hi, rea_lo = split(on_diagonal(react_ref[...]))
    both_hi = jnp.concatenate([row_hi, col_hi], axis=1)
    w1[0:two] = both_hi
    w1[two:2 * two] = both_hi
    w2[...] = jnp.concatenate([row_lo, col_lo], axis=1)
    w3[0:two] = jnp.concatenate([rea_hi, rea_lo], axis=1)
    w3[two:2 * two] = jnp.concatenate([rea_hi, jnp.zeros_like(rea_lo)], axis=1)

    k = rate_ref.shape[0]
    part = k8 + 8
    rates = jnp.concatenate([rate_ref[...], rate_ref[...]], axis=1)
    heats = jnp.concatenate([heat_ref[...], heat_ref[...]], axis=1)
    wc[...] = jnp.zeros_like(wc)
    for s in range(2):
        mine = (lanes((1, two)) < c) if s == 0 else (lanes((1, two)) >= c)
        wc[s * part:s * part + k, 0:two] = jnp.where(mine, rates, 0.0)
        wc[s * part + k8:s * part + k8 + 1, two:2 * two] = jnp.where(mine, 1.0, 0.0)
        wc[s * part + k8 + 1:s * part + k8 + 2, 2 * two:3 * two] = jnp.where(mine, heats, 0.0)
    tables = jnp.concatenate(split(wc[...]), axis=0)
    classes, slots = rows_of((k8, w)), rows_of((8, w))

    def cells(p, carry):
        parts = []
        for s in range(2):
            at = pl.ds(p + s * p_all, 1)
            alive = 1.0 - break_ref[at, :].astype(F32)
            lit = alive * lit_ref[at, :].astype(F32)
            parts.append(jnp.where(fuel_ref[at, :] == classes, alive, 0.0))
            parts.append(jnp.where(slots == 0, alive, jnp.where(slots == 1, lit, 0.0)))
        tall = jnp.concatenate(parts + parts, axis=0)
        terms = dot(tall.T.astype(BF16), tables)
        coef[p] = terms[:, 0:two]
        burn[p] = terms[:, two:2 * two]
        heat[p] = terms[:, 2 * two:3 * two]
        return carry

    lax.fori_loop(0, p_all, cells, 0, unroll=4)

    def spreads(x):
        hi, lo = split(x)
        return dot(jnp.concatenate([hi, lo], axis=1), w1[...]) + dot(hi, w2[...])

    def pointwise(cur, second):
        def body(b, carry):
            at = pl.ds(b * BLOCK, BLOCK)
            x = cur[at].reshape(BLOCK * w, two)
            g = spreads(x)
            g_row, g_col = g[:, :two], g[:, two:]
            hi, lo = split(jnp.tanh(x))
            both = dot(jnp.concatenate([hi, lo], axis=1), w3[...])
            burning = both[:, :two] + both[:, two:]
            flat = lambda ref: ref[at].reshape(BLOCK * w, two)
            fire = flat(burn) * burning + flat(heat) - 2.0 * (flat(coef) * (g_row + g_col)) + 0.5 * x
            if second:
                fire = 0.5 * (fire + flat(v))
            gr[pl.ds(b * BLOCK + 1, BLOCK)] = g_row.reshape(BLOCK, w, two)
            gc[at, PAD:PAD + w] = g_col.reshape(BLOCK, w, two)
            local[at] = fire.reshape(BLOCK, w, two)
            return carry

        lax.fori_loop(0, p_all // BLOCK, body, 0)

    def halo(slot):
        stacked = jnp.concatenate([recv_row[slot, 0], recv_row[slot, 1], recv_col[slot, 0], recv_col[slot, 1]], axis=0)
        g = spreads(stacked)
        below, above = g[0:half, :two], g[half:w, :two]
        last, top = gr[p_all], gr[1]
        wide_first = lanes((w, two)) < c
        over = jnp.concatenate([above, pltpu.roll(above, c, axis=1)], axis=0)
        under = jnp.concatenate([pltpu.roll(below, c, axis=1), below], axis=0)
        gr[0] = jnp.where(wide_first, over, pltpu.roll(last, c, axis=1))
        gr[p_all + 1] = jnp.where(wide_first, pltpu.roll(top, c, axis=1), under)
        flat = gc.reshape(p_all * (w + 2 * PAD), two)
        flat[pl.ds(PAD + w, p_all, stride=w + 2 * PAD), :] = g[w:w + p_all, two:]
        flat[pl.ds(PAD - 1, p_all, stride=w + 2 * PAD), :] = g[w + p_all:w + 2 * p_all, two:]

    def combine(slot, target, second, last):
        def value(p):
            near = (gr[p] + gr[p + 2]) + (gc[p, PAD - 1:PAD - 1 + w] + gc[p, PAD + 1:PAD + 1 + w])
            if second:
                near = 0.5 * near
            return local[p] + coef[p] * near

        def edge(at):
            near = (column(gr, at)(0) + column(gr, at)(2)) + (column(gc, PAD - 1 + at)(0) + column(gc, PAD + 1 + at)(0))
            if second:
                near = 0.5 * near
            return column(local, at)(0) + column(coef, at)(0) * near

        top, bottom = value(0), value(p_all - 1)
        target[0] = top
        target[p_all - 1] = bottom

        def edges():
            send_rows(slot, top, bottom)
            send_cols(slot, edge(0), edge(w - 1))

        if last is None:
            edges()
        else:
            pl.when(jnp.logical_not(last))(edges)

        def body(p, carry):
            target[p] = value(p)
            return carry

        lax.fori_loop(1, p_all - 1, body, 0, unroll=2)

    def step(i, carry):
        pointwise(v, False)
        finish(0)
        halo(0)
        combine(1, mid, False, None)
        pointwise(mid, True)
        finish(1)
        halo(1)
        combine(0, v, True, i == ITERS - 1)
        return carry

    lax.fori_loop(0, ITERS, step, 0)

    def turn_out(p, carry):
        tall = v[p].T
        out_ref[pl.ds(p, c, stride=h), :] = tall[:c]
        out_ref[pl.ds(p + p_all, c, stride=h), :] = tall[c:]
        return carry

    lax.fori_loop(0, p_all, turn_out, 0, unroll=4)


def per_device(n_row, n_col, fire_state, fuel_class, firebreak, ignition, spread_rate, spread_rows, spread_cols, reaction, ignition_heat):
    c, h, w = fire_state.shape
    k = spread_rate.shape[0]
    k8 = -(-k // 8) * 8
    p_all, two = h // 2, 2 * c
    vmem = pl.BlockSpec(memory_space=pltpu.VMEM)
    field = pltpu.VMEM((p_all, w, two), F32)
    out = pl.pallas_call(
        functools.partial(kernel, (n_row, n_col, c, h, w, k8)),
        out_shape=jax.ShapeDtypeStruct((c * h, w), F32),
        in_specs=[vmem] * 9,
        out_specs=vmem,
        scratch_shapes=[
            field, field, field, field, field, field,
            pltpu.VMEM((p_all + 2, w, two), F32),
            pltpu.VMEM((p_all, w + 2 * PAD, two), F32),
            pltpu.VMEM((2 * two, 2 * two), BF16),
            pltpu.VMEM((two, 2 * two), BF16),
            pltpu.VMEM((2 * two, 2 * two), BF16),
            pltpu.VMEM((2 * (k8 + 8), 3 * two), F32),
            pltpu.VMEM((2, 2, w // 2, two), F32),
            pltpu.VMEM((2, 2, p_all, two), F32),
            pltpu.VMEM((2, 2, w // 2, two), F32),
            pltpu.VMEM((2, 2, p_all, two), F32),
            pltpu.SemaphoreType.DMA((2, 4)),
            pltpu.SemaphoreType.DMA((2, 4)),
        ],
        compiler_params=pltpu.CompilerParams(collective_id=0, has_side_effects=True, vmem_limit_bytes=48 * 1024 * 1024),
    )(
        fire_state.reshape(c * h, w), fuel_class, firebreak, ignition,
        spread_rate, spread_rows, spread_cols, reaction, ignition_heat.reshape(1, c),
    )
    return out.reshape(c, h, w)


def solution(mesh):
    grid = P("row", "col")
    field = P(None, "row", "col")
    return jax.shard_map(
        functools.partial(per_device, mesh.shape["row"], mesh.shape["col"]),
        mesh=mesh,
        in_specs=(field, grid, grid, grid, P(), P(), P(), P(), P()),
        out_specs=field,
        check_vma=False,
    )
```

```python
import functools

import jax
import jax.numpy as jnp
from jax import lax
from jax.experimental import pallas as pl
from jax.experimental.pallas import tpu as pltpu
from jax.sharding import PartitionSpec as P

ITERS = 4
PAD = 8
BLOCK = 4
BF16, F32 = jnp.bfloat16, jnp.float32
MESH = pl.DeviceIdType.MESH


def split(x):
    high = x.astype(BF16)
    return high, (x - high.astype(F32)).astype(BF16)


def dot(a, b):
    return jnp.dot(a, b, preferred_element_type=F32)


def lanes(shape):
    return lax.broadcasted_iota(jnp.int32, shape, 1)


def rows_of(shape):
    return lax.broadcasted_iota(jnp.int32, shape, 0)


def on_diagonal(matrix):
    c = matrix.shape[0]
    turned = matrix.T
    wide = jnp.concatenate([turned, turned], axis=1)
    first = lanes(wide.shape) < c
    return jnp.concatenate([jnp.where(first, wide, 0.0), jnp.where(first, 0.0, wide)], axis=0)


def kernel(
    dims,
    x_hbm, fuel_hbm, break_hbm, lit_hbm, rate_hbm, srow_hbm, scol_hbm, react_hbm, heat_hbm,
    out_ref,
    x_ref, fuel_ref, break_ref, lit_ref, rate_ref, srow_ref, scol_ref, react_ref, heat_ref, ends_ref, load_sem,
    v, mid, local, coef, burn, heat, gr, gc, w1, w2, w3, wc, send_row, send_col, recv_row, recv_col, send_sem, recv_sem,
):
    n_row, n_col, c, h, w, k8 = dims
    p_all, half = h // 2, w // 2
    two = 2 * c
    r, q = lax.axis_index("row"), lax.axis_index("col")
    has_up, has_down = r > 0, r < n_row - 1
    has_left, has_right = q > 0, q < n_col - 1
    partner = ({"row": r - 1}, {"row": r + 1}, {"col": q - 1}, {"col": q + 1})
    sends = (has_up, has_down, has_left, has_right)
    takes = (has_down, has_up, has_right, has_left)

    def load(n, src, dst):
        return pltpu.make_async_copy(src, dst, load_sem.at[n])

    end_loads = [load(0, x_hbm.at[:, 0, :], ends_ref.at[0]), load(1, x_hbm.at[:, h - 1, :], ends_ref.at[1])]
    weight_loads = [load(2, srow_hbm, srow_ref), load(3, scol_hbm, scol_ref), load(4, react_hbm, react_ref)]
    field_load = load(5, x_hbm, x_ref.reshape(c, h, w))
    cell_loads = [
        load(6, fuel_hbm, fuel_ref), load(7, break_hbm, break_ref), load(8, lit_hbm, lit_ref),
        load(9, rate_hbm, rate_ref), load(10, heat_hbm, heat_ref),
    ]
    for one in end_loads + weight_loads + [field_load] + cell_loads:
        one.start()

    recv_row[...] = jnp.zeros_like(recv_row)
    recv_col[...] = jnp.zeros_like(recv_col)
    barrier = pltpu.get_barrier_semaphore()
    for d in range(4):
        @pl.when(sends[d])
        def _(d=d):
            pl.semaphore_signal(barrier, inc=1, device_id=partner[d], device_id_type=MESH)

    def copy(slot, d):
        src, dst = (send_row, recv_row) if d < 2 else (send_col, recv_col)
        return pltpu.make_async_remote_copy(
            src_ref=src.at[slot, d % 2],
            dst_ref=dst.at[slot, d % 2],
            send_sem=send_sem.at[slot, d],
            recv_sem=recv_sem.at[slot, d],
            device_id=partner[d],
            device_id_type=MESH,
        )

    def start(slot, d):
        @pl.when(sends[d])
        def _():
            copy(slot, d).start()

    def finish(slot):
        for d in range(4):
            @pl.when(sends[d])
            def _(d=d):
                copy(slot, d).wait_send()
        for d in range(4):
            @pl.when(takes[d])
            def _(d=d):
                copy(slot, d).wait_recv()

    first_half = lanes((half, two)) < c

    def send_rows(slot, top, bottom):
        send_row[slot, 0] = jnp.where(first_half, top[:half], pltpu.roll(top[half:], c, axis=1))
        send_row[slot, 1] = jnp.where(first_half, pltpu.roll(bottom[:half], c, axis=1), bottom[half:])
        odd = lax.rem(r, 2) == 1

        @pl.when(odd)
        def _():
            start(slot, 1)
            start(slot, 0)

        @pl.when(jnp.logical_not(odd))
        def _():
            start(slot, 0)
            start(slot, 1)

    def turn_in(p):
        tall = jnp.concatenate([x_ref[pl.ds(p, c, stride=h), :], x_ref[pl.ds(p + p_all, c, stride=h), :]], axis=0)
        v[p] = tall.T

    def turn_in_loop(p, carry):
        turn_in(p)
        return carry

    def column(ref, at):
        size = ref.shape[1]
        flat = ref.reshape(ref.shape[0] * size, two)
        return lambda p: flat[pl.ds(p * size + at, p_all, stride=size), :]

    def send_cols(slot, left, right):
        send_col[slot, 0] = left
        send_col[slot, 1] = right
        start(slot, 2)
        start(slot, 3)

    n_near = sum(s.astype(jnp.int32) for s in sends)
    for one in end_loads:
        one.wait()
    ends = jnp.concatenate([ends_ref[0], ends_ref[1]], axis=0).T
    pl.semaphore_wait(barrier, n_near)
    send_rows(0, ends, ends)

    for one in weight_loads:
        one.wait()
    eye = (rows_of((two, two)) == lanes((two, two))).astype(F32)
    row_hi, row_lo = split(eye + on_diagonal(srow_ref[...]))
    col_hi, col_lo = split(eye + on_diagonal(scol_ref[...]))
    rea_hi, rea_lo = split(on_diagonal(react_ref[...]))
    both_hi = jnp.concatenate([row_hi, col_hi], axis=1)
    w1[0:two] = both_hi
    w1[two:2 * two] = both_hi
    w2[...] = jnp.concatenate([row_lo, col_lo], axis=1)
    w3[0:two] = jnp.concatenate([rea_hi, rea_lo], axis=1)
    w3[two:2 * two] = jnp.concatenate([rea_hi, jnp.zeros_like(rea_lo)], axis=1)

    field_load.wait()
    lax.fori_loop(0, p_all, turn_in_loop, 0, unroll=4)
    send_cols(0, column(v, 0)(0), column(v, w - 1)(0))
    for one in cell_loads:
        one.wait()

    k = rate_ref.shape[0]
    part = k8 + 8
    rates = jnp.concatenate([rate_ref[...], rate_ref[...]], axis=1)
    heats = jnp.concatenate([heat_ref[...], heat_ref[...]], axis=1)
    wc[...] = jnp.zeros_like(wc)
    for s in range(2):
        mine = (lanes((1, two)) < c) if s == 0 else (lanes((1, two)) >= c)
        wc[s * part:s * part + k, 0:two] = jnp.where(mine, rates, 0.0)
        wc[s * part + k8:s * part + k8 + 1, two:2 * two] = jnp.where(mine, 1.0, 0.0)
        wc[s * part + k8 + 1:s * part + k8 + 2, 2 * two:3 * two] = jnp.where(mine, heats, 0.0)
    tables = jnp.concatenate(split(wc[...]), axis=0)
    classes, slots = rows_of((k8, w)), rows_of((8, w))

    def cells(p, carry):
        parts = []
        for s in range(2):
            at = pl.ds(p + s * p_all, 1)
            alive = 1.0 - break_ref[at, :].astype(F32)
            lit = alive * lit_ref[at, :].astype(F32)
            parts.append(jnp.where(fuel_ref[at, :] == classes, alive, 0.0))
            parts.append(jnp.where(slots == 0, alive, jnp.where(slots == 1, lit, 0.0)))
        tall = jnp.concatenate(parts + parts, axis=0)
        terms = dot(tall.T.astype(BF16), tables)
        coef[p] = terms[:, 0:two]
        burn[p] = terms[:, two:2 * two]
        heat[p] = terms[:, 2 * two:3 * two]
        return carry

    lax.fori_loop(0, p_all, cells, 0, unroll=4)

    def spreads(x):
        hi, lo = split(x)
        return dot(jnp.concatenate([hi, lo], axis=1), w1[...]) + dot(hi, w2[...])

    def pointwise(cur, second):
        def body(b, carry):
            at = pl.ds(b * BLOCK, BLOCK)
            x = cur[at].reshape(BLOCK * w, two)
            g = spreads(x)
            g_row, g_col = g[:, :two], g[:, two:]
            hi, lo = split(jnp.tanh(x))
            both = dot(jnp.concatenate([hi, lo], axis=1), w3[...])
            burning = both[:, :two] + both[:, two:]
            flat = lambda ref: ref[at].reshape(BLOCK * w, two)
            fire = flat(burn) * burning + flat(heat) - 2.0 * (flat(coef) * (g_row + g_col)) + 0.5 * x
            if second:
                fire = 0.5 * (fire + flat(v))
            gr[pl.ds(b * BLOCK + 1, BLOCK)] = g_row.reshape(BLOCK, w, two)
            gc[at, PAD:PAD + w] = g_col.reshape(BLOCK, w, two)
            local[at] = fire.reshape(BLOCK, w, two)
            return carry

        lax.fori_loop(0, p_all // BLOCK, body, 0)

    def halo(slot):
        stacked = jnp.concatenate([recv_row[slot, 0], recv_row[slot, 1], recv_col[slot, 0], recv_col[slot, 1]], axis=0)
        g = spreads(stacked)
        below, above = g[0:half, :two], g[half:w, :two]
        last, top = gr[p_all], gr[1]
        wide_first = lanes((w, two)) < c
        over = jnp.concatenate([above, pltpu.roll(above, c, axis=1)], axis=0)
        under = jnp.concatenate([pltpu.roll(below, c, axis=1), below], axis=0)
        gr[0] = jnp.where(wide_first, over, pltpu.roll(last, c, axis=1))
        gr[p_all + 1] = jnp.where(wide_first, pltpu.roll(top, c, axis=1), under)
        flat = gc.reshape(p_all * (w + 2 * PAD), two)
        flat[pl.ds(PAD + w, p_all, stride=w + 2 * PAD), :] = g[w:w + p_all, two:]
        flat[pl.ds(PAD - 1, p_all, stride=w + 2 * PAD), :] = g[w + p_all:w + 2 * p_all, two:]

    def combine(slot, target, second, last):
        def value(p):
            near = (gr[p] + gr[p + 2]) + (gc[p, PAD - 1:PAD - 1 + w] + gc[p, PAD + 1:PAD + 1 + w])
            if second:
                near = 0.5 * near
            return local[p] + coef[p] * near

        def edge(at):
            near = (column(gr, at)(0) + column(gr, at)(2)) + (column(gc, PAD - 1 + at)(0) + column(gc, PAD + 1 + at)(0))
            if second:
                near = 0.5 * near
            return column(local, at)(0) + column(coef, at)(0) * near

        top, bottom = value(0), value(p_all - 1)
        target[0] = top
        target[p_all - 1] = bottom

        def edges():
            send_rows(slot, top, bottom)
            send_cols(slot, edge(0), edge(w - 1))

        if last is None:
            edges()
        else:
            pl.when(jnp.logical_not(last))(edges)

        def body(p, carry):
            target[p] = value(p)
            return carry

        lax.fori_loop(1, p_all - 1, body, 0, unroll=2)

    def step(i, carry):
        pointwise(v, False)
        finish(0)
        halo(0)
        combine(1, mid, False, None)
        pointwise(mid, True)
        finish(1)
        halo(1)
        combine(0, v, True, i == ITERS - 1)
        return carry

    lax.fori_loop(0, ITERS, step, 0)

    def turn_out(p, carry):
        tall = v[p].T
        out_ref[pl.ds(p, c, stride=h), :] = tall[:c]
        out_ref[pl.ds(p + p_all, c, stride=h), :] = tall[c:]
        return carry

    lax.fori_loop(0, p_all, turn_out, 0, unroll=4)


def per_device(n_row, n_col, fire_state, fuel_class, firebreak, ignition, spread_rate, spread_rows, spread_cols, reaction, ignition_heat):
    c, h, w = fire_state.shape
    k = spread_rate.shape[0]
    k8 = -(-k // 8) * 8
    p_all, two = h // 2, 2 * c
    vmem = pl.BlockSpec(memory_space=pltpu.VMEM)
    field = pltpu.VMEM((p_all, w, two), F32)
    out = pl.pallas_call(
        functools.partial(kernel, (n_row, n_col, c, h, w, k8)),
        out_shape=jax.ShapeDtypeStruct((c * h, w), F32),
        in_specs=[pl.BlockSpec(memory_space=pltpu.HBM)] * 9,
        out_specs=vmem,
        scratch_shapes=[
            pltpu.VMEM((c * h, w), F32),
            pltpu.VMEM((h, w), jnp.int32), pltpu.VMEM((h, w), jnp.int32), pltpu.VMEM((h, w), jnp.int32),
            pltpu.VMEM(spread_rate.shape, F32),
            pltpu.VMEM((c, c), F32), pltpu.VMEM((c, c), F32), pltpu.VMEM((c, c), F32),
            pltpu.VMEM((1, c), F32),
            pltpu.VMEM((2, c, w), F32),
            pltpu.SemaphoreType.DMA((11,)),
            field, field, field, field, field, field,
            pltpu.VMEM((p_all + 2, w, two), F32),
            pltpu.VMEM((p_all, w + 2 * PAD, two), F32),
            pltpu.VMEM((2 * two, 2 * two), BF16),
            pltpu.VMEM((two, 2 * two), BF16),
            pltpu.VMEM((2 * two, 2 * two), BF16),
            pltpu.VMEM((2 * (k8 + 8), 3 * two), F32),
            pltpu.VMEM((2, 2, w // 2, two), F32),
            pltpu.VMEM((2, 2, p_all, two), F32),
            pltpu.VMEM((2, 2, w // 2, two), F32),
            pltpu.VMEM((2, 2, p_all, two), F32),
            pltpu.SemaphoreType.DMA((2, 4)),
            pltpu.SemaphoreType.DMA((2, 4)),
        ],
        compiler_params=pltpu.CompilerParams(collective_id=0, has_side_effects=True, vmem_limit_bytes=56 * 1048576),
    )(
        fire_state, fuel_class, firebreak, ignition,
        spread_rate, spread_rows, spread_cols, reaction, ignition_heat.reshape(1, c),
    )
    return out.reshape(c, h, w)


def solution(mesh):
    grid = P("row", "col")
    field = P(None, "row", "col")
    return jax.shard_map(
        functools.partial(per_device, mesh.shape["row"], mesh.shape["col"]),
        mesh=mesh,
        in_specs=(field, grid, grid, grid, P(), P(), P(), P(), P()),
        out_specs=field,
        check_vma=False,
    )
```

```python
import functools

import jax
import jax.numpy as jnp
from jax import lax
from jax.experimental import pallas as pl
from jax.experimental.pallas import tpu as pltpu
from jax.sharding import PartitionSpec as P

ITERS = 4
PAD = 8
BLOCK = 12
BF16, F32 = jnp.bfloat16, jnp.float32
MESH = pl.DeviceIdType.MESH


def split(x):
    high = x.astype(BF16)
    return high, (x - high.astype(F32)).astype(BF16)


def dot(a, b):
    return jnp.dot(a, b, preferred_element_type=F32)


def lanes(shape):
    return lax.broadcasted_iota(jnp.int32, shape, 1)


def rows_of(shape):
    return lax.broadcasted_iota(jnp.int32, shape, 0)


def on_diagonal(matrix):
    c = matrix.shape[0]
    turned = matrix.T
    wide = jnp.concatenate([turned, turned], axis=1)
    first = lanes(wide.shape) < c
    return jnp.concatenate([jnp.where(first, wide, 0.0), jnp.where(first, 0.0, wide)], axis=0)


def kernel(
    dims,
    x_hbm, fuel_hbm, break_hbm, lit_hbm, rate_hbm, srow_hbm, scol_hbm, react_hbm, heat_hbm,
    out_ref,
    x_ref, fuel_ref, break_ref, lit_ref, rate_ref, srow_ref, scol_ref, react_ref, heat_ref, ends_ref, load_sem,
    v, mid, local, coef, burn, heat, gr, gc, w1, w2, w3, wc, send_row, send_col, recv_row, recv_col, send_sem, recv_sem,
):
    n_row, n_col, c, h, w, k8 = dims
    p_all, half = h // 2, w // 2
    two = 2 * c
    r, q = lax.axis_index("row"), lax.axis_index("col")
    has_up, has_down = r > 0, r < n_row - 1
    has_left, has_right = q > 0, q < n_col - 1
    partner = ({"row": r - 1}, {"row": r + 1}, {"col": q - 1}, {"col": q + 1})
    sends = (has_up, has_down, has_left, has_right)
    takes = (has_down, has_up, has_right, has_left)

    def load(n, src, dst):
        return pltpu.make_async_copy(src, dst, load_sem.at[n])

    end_loads = [load(0, x_hbm.at[:, 0, :], ends_ref.at[0]), load(1, x_hbm.at[:, h - 1, :], ends_ref.at[1])]
    weight_loads = [load(2, srow_hbm, srow_ref), load(3, scol_hbm, scol_ref), load(4, react_hbm, react_ref)]
    field_load = load(5, x_hbm, x_ref.reshape(c, h, w))
    cell_loads = [
        load(6, fuel_hbm, fuel_ref), load(7, break_hbm, break_ref), load(8, lit_hbm, lit_ref),
        load(9, rate_hbm, rate_ref), load(10, heat_hbm, heat_ref),
    ]
    for one in end_loads + weight_loads + [field_load] + cell_loads:
        one.start()

    recv_row[...] = jnp.zeros_like(recv_row)
    recv_col[...] = jnp.zeros_like(recv_col)
    barrier = pltpu.get_barrier_semaphore()
    for d in range(4):
        @pl.when(sends[d])
        def _(d=d):
            pl.semaphore_signal(barrier, inc=1, device_id=partner[d], device_id_type=MESH)

    def copy(slot, d):
        src, dst = (send_row, recv_row) if d < 2 else (send_col, recv_col)
        return pltpu.make_async_remote_copy(
            src_ref=src.at[slot, d % 2],
            dst_ref=dst.at[slot, d % 2],
            send_sem=send_sem.at[slot, d],
            recv_sem=recv_sem.at[slot, d],
            device_id=partner[d],
            device_id_type=MESH,
        )

    def start(slot, d):
        @pl.when(sends[d])
        def _():
            copy(slot, d).start()

    def sent(slot):
        for d in range(4):
            @pl.when(sends[d])
            def _(d=d):
                copy(slot, d).wait_send()

    def arrived(slot):
        for d in range(4):
            @pl.when(takes[d])
            def _(d=d):
                copy(slot, d).wait_recv()

    first_half = lanes((half, two)) < c

    def send_rows(slot, top, bottom):
        send_row[slot, 0] = jnp.where(first_half, top[:half], pltpu.roll(top[half:], c, axis=1))
        send_row[slot, 1] = jnp.where(first_half, pltpu.roll(bottom[:half], c, axis=1), bottom[half:])
        odd = lax.rem(r, 2) == 1

        @pl.when(odd)
        def _():
            start(slot, 1)
            start(slot, 0)

        @pl.when(jnp.logical_not(odd))
        def _():
            start(slot, 0)
            start(slot, 1)

    def turn_in(p):
        tall = jnp.concatenate([x_ref[pl.ds(p, c, stride=h), :], x_ref[pl.ds(p + p_all, c, stride=h), :]], axis=0)
        v[p] = tall.T

    def turn_in_loop(p, carry):
        turn_in(p)
        return carry

    def column(ref, at):
        size = ref.shape[1]
        flat = ref.reshape(ref.shape[0] * size, two)
        return lambda p: flat[pl.ds(p * size + at, p_all, stride=size), :]

    def send_cols(slot, left, right):
        send_col[slot, 0] = left
        send_col[slot, 1] = right
        start(slot, 2)
        start(slot, 3)

    n_near = sum(s.astype(jnp.int32) for s in sends)
    for one in end_loads:
        one.wait()
    ends = jnp.concatenate([ends_ref[0], ends_ref[1]], axis=0).T
    pl.semaphore_wait(barrier, n_near)
    send_rows(0, ends, ends)

    for one in weight_loads:
        one.wait()
    eye = (rows_of((two, two)) == lanes((two, two))).astype(F32)
    row_hi, row_lo = split(eye + on_diagonal(srow_ref[...]))
    col_hi, col_lo = split(eye + on_diagonal(scol_ref[...]))
    rea_hi, rea_lo = split(on_diagonal(react_ref[...]))
    both_hi = jnp.concatenate([row_hi, col_hi], axis=1)
    w1[0:two] = both_hi
    w1[two:2 * two] = both_hi
    w2[...] = jnp.concatenate([row_lo, col_lo], axis=1)
    w3[0:two] = jnp.concatenate([rea_hi, rea_lo], axis=1)
    w3[two:2 * two] = jnp.concatenate([rea_hi, jnp.zeros_like(rea_lo)], axis=1)

    field_load.wait()
    lax.fori_loop(0, p_all, turn_in_loop, 0, unroll=4)
    send_cols(0, column(v, 0)(0), column(v, w - 1)(0))
    for one in cell_loads:
        one.wait()

    k = rate_ref.shape[0]
    part = k8 + 8
    rates = jnp.concatenate([rate_ref[...], rate_ref[...]], axis=1)
    heats = jnp.concatenate([heat_ref[...], heat_ref[...]], axis=1)
    wc[...] = jnp.zeros_like(wc)
    for s in range(2):
        mine = (lanes((1, two)) < c) if s == 0 else (lanes((1, two)) >= c)
        wc[s * part:s * part + k, 0:two] = jnp.where(mine, rates, 0.0)
        wc[s * part + k8:s * part + k8 + 1, two:2 * two] = jnp.where(mine, 1.0, 0.0)
        wc[s * part + k8 + 1:s * part + k8 + 2, 2 * two:3 * two] = jnp.where(mine, heats, 0.0)
    tables = jnp.concatenate(split(wc[...]), axis=0)
    classes, slots = rows_of((k8, w)), rows_of((8, w))

    def cells(p, carry):
        parts = []
        for s in range(2):
            at = pl.ds(p + s * p_all, 1)
            alive = 1.0 - break_ref[at, :].astype(F32)
            lit = alive * lit_ref[at, :].astype(F32)
            parts.append(jnp.where(fuel_ref[at, :] == classes, alive, 0.0))
            parts.append(jnp.where(slots == 0, alive, jnp.where(slots == 1, lit, 0.0)))
        tall = jnp.concatenate(parts + parts, axis=0)
        terms = dot(tall.T.astype(BF16), tables)
        coef[p] = terms[:, 0:two]
        burn[p] = terms[:, two:2 * two]
        heat[p] = terms[:, 2 * two:3 * two]
        return carry

    lax.fori_loop(0, p_all, cells, 0, unroll=4)

    def spreads(x):
        hi, lo = split(x)
        return dot(jnp.concatenate([hi, lo], axis=1), w1[...]) + dot(hi, w2[...])

    def pointwise(cur, second):
        def body(b, carry):
            at = pl.ds(b * BLOCK, BLOCK)
            x = cur[at].reshape(BLOCK * w, two)
            g = spreads(x)
            g_row, g_col = g[:, :two], g[:, two:]
            hi, lo = split(jnp.tanh(x))
            both = dot(jnp.concatenate([hi, lo], axis=1), w3[...])
            burning = both[:, :two] + both[:, two:]
            flat = lambda ref: ref[at].reshape(BLOCK * w, two)
            fire = flat(burn) * burning + flat(heat) - 2.0 * (flat(coef) * (g_row + g_col)) + 0.5 * x
            if second:
                fire = 0.5 * (fire + flat(v))
            gr[pl.ds(b * BLOCK + 1, BLOCK)] = g_row.reshape(BLOCK, w, two)
            gc[at, PAD:PAD + w] = g_col.reshape(BLOCK, w, two)
            local[at] = fire.reshape(BLOCK, w, two)
            return carry

        lax.fori_loop(0, p_all // BLOCK, body, 0)

    def halo(slot):
        stacked = jnp.concatenate([recv_row[slot, 0], recv_row[slot, 1], recv_col[slot, 0], recv_col[slot, 1]], axis=0)
        g = spreads(stacked)
        below, above = g[0:half, :two], g[half:w, :two]
        last, top = gr[p_all], gr[1]
        wide_first = lanes((w, two)) < c
        over = jnp.concatenate([above, pltpu.roll(above, c, axis=1)], axis=0)
        under = jnp.concatenate([pltpu.roll(below, c, axis=1), below], axis=0)
        gr[0] = jnp.where(wide_first, over, pltpu.roll(last, c, axis=1))
        gr[p_all + 1] = jnp.where(wide_first, pltpu.roll(top, c, axis=1), under)
        flat = gc.reshape(p_all * (w + 2 * PAD), two)
        flat[pl.ds(PAD + w, p_all, stride=w + 2 * PAD), :] = g[w:w + p_all, two:]
        flat[pl.ds(PAD - 1, p_all, stride=w + 2 * PAD), :] = g[w + p_all:w + 2 * p_all, two:]

    def combine(slot, target, second, last):
        def value(p):
            near = (gr[p] + gr[p + 2]) + (gc[p, PAD - 1:PAD - 1 + w] + gc[p, PAD + 1:PAD + 1 + w])
            if second:
                near = 0.5 * near
            return local[p] + coef[p] * near

        def edge(at):
            near = (column(gr, at)(0) + column(gr, at)(2)) + (column(gc, PAD - 1 + at)(0) + column(gc, PAD + 1 + at)(0))
            if second:
                near = 0.5 * near
            return column(local, at)(0) + column(coef, at)(0) * near

        top, bottom = value(0), value(p_all - 1)
        target[0] = top
        target[p_all - 1] = bottom

        def edges():
            send_rows(slot, top, bottom)
            send_cols(slot, edge(0), edge(w - 1))

        if last is None:
            edges()
        else:
            pl.when(jnp.logical_not(last))(edges)

        def body(p, carry):
            target[p] = value(p)
            return carry

        lax.fori_loop(1, p_all - 1, body, 0, unroll=2)

    def step(i, carry):
        pointwise(v, False)
        arrived(0)
        halo(0)
        combine(1, mid, False, None)
        pointwise(mid, True)
        arrived(1)
        halo(1)
        sent(0)
        combine(0, v, True, i == ITERS - 1)
        sent(1)
        return carry

    lax.fori_loop(0, ITERS, step, 0)

    def turn_out(p, carry):
        tall = v[p].T
        out_ref[pl.ds(p, c, stride=h), :] = tall[:c]
        out_ref[pl.ds(p + p_all, c, stride=h), :] = tall[c:]
        return carry

    lax.fori_loop(0, p_all, turn_out, 0, unroll=4)


def per_device(n_row, n_col, fire_state, fuel_class, firebreak, ignition, spread_rate, spread_rows, spread_cols, reaction, ignition_heat):
    c, h, w = fire_state.shape
    k = spread_rate.shape[0]
    k8 = -(-k // 8) * 8
    p_all, two = h // 2, 2 * c
    vmem = pl.BlockSpec(memory_space=pltpu.VMEM)
    field = pltpu.VMEM((p_all, w, two), F32)
    out = pl.pallas_call(
        functools.partial(kernel, (n_row, n_col, c, h, w, k8)),
        out_shape=jax.ShapeDtypeStruct((c * h, w), F32),
        in_specs=[pl.BlockSpec(memory_space=pltpu.HBM)] * 9,
        out_specs=vmem,
        scratch_shapes=[
            pltpu.VMEM((c * h, w), F32),
            pltpu.VMEM((h, w), jnp.int32), pltpu.VMEM((h, w), jnp.int32), pltpu.VMEM((h, w), jnp.int32),
            pltpu.VMEM(spread_rate.shape, F32),
            pltpu.VMEM((c, c), F32), pltpu.VMEM((c, c), F32), pltpu.VMEM((c, c), F32),
            pltpu.VMEM((1, c), F32),
            pltpu.VMEM((2, c, w), F32),
            pltpu.SemaphoreType.DMA((11,)),
            field, field, field, field, field, field,
            pltpu.VMEM((p_all + 2, w, two), F32),
            pltpu.VMEM((p_all, w + 2 * PAD, two), F32),
            pltpu.VMEM((2 * two, 2 * two), BF16),
            pltpu.VMEM((two, 2 * two), BF16),
            pltpu.VMEM((2 * two, 2 * two), BF16),
            pltpu.VMEM((2 * (k8 + 8), 3 * two), F32),
            pltpu.VMEM((2, 2, w // 2, two), F32),
            pltpu.VMEM((2, 2, p_all, two), F32),
            pltpu.VMEM((2, 2, w // 2, two), F32),
            pltpu.VMEM((2, 2, p_all, two), F32),
            pltpu.SemaphoreType.DMA((2, 4)),
            pltpu.SemaphoreType.DMA((2, 4)),
        ],
        compiler_params=pltpu.CompilerParams(collective_id=0, has_side_effects=True, vmem_limit_bytes=56 * 1048576),
    )(
        fire_state, fuel_class, firebreak, ignition,
        spread_rate, spread_rows, spread_cols, reaction, ignition_heat.reshape(1, c),
    )
    return out.reshape(c, h, w)


def solution(mesh):
    grid = P("row", "col")
    field = P(None, "row", "col")
    return jax.shard_map(
        functools.partial(per_device, mesh.shape["row"], mesh.shape["col"]),
        mesh=mesh,
        in_specs=(field, grid, grid, grid, P(), P(), P(), P(), P()),
        out_specs=field,
        check_vma=False,
    )
```
